32 devices in a mesh: grp: 2 (over y), zt: 4 (over x, core), xy: 4 (over z).
Axes of the slice: x: 2, y: 2, z: 4, core: 2. Of those that a mesh axis runs over, the one named last changes fastest.
Arguments:
- source: float32 [2, 2, 3, 8, 16, 128], P('grp', None, None, 'xy', 'zt'), may hold values from -6 to 6
- links: float32 [4, 2, 3, 3, 8, 16, 128], P('grp', None, None, None, 'xy', 'zt'), may hold values from -2 to 2
- shifts: float32 [12], replicated, may hold values from 0.01 to 0.5
- residues: float32 [12], replicated, may hold values from 0.05 to 0.5
- mass: float32 [1], replicated, may hold values from 0.1 to 0.5
Outputs:
- rational: float32 [2, 2, 3, 8, 16, 128], P('grp', None, None, 'xy', 'zt')
- action: float32 [1], replicated
The draws below stay inside these ranges and needn't reach their ends.
All inputs are finite; a program needn't handle non-finite values.
Results may differ from the reference program's by a relative error of at most 0.0003.
Values sent between devices are 32-bit elements; how exact they have to be, the bound alone decides.
A program may use at most 64 MiB of HBM per device.

```python
import math
import jax
import jax.numpy as jnp

NY = 2
NZ = 64
NSHIFT = 12
ITERS = 8
PF = 2
NX = 8
NT = 16


def levels(own_key, extent, split, smallest, high):
    def one(position, shards_of):
        draws = jax.random.uniform(jax.random.fold_in(jax.random.fold_in(own_key, 6), position), (shards_of,), jnp.float32, smallest / len(split), high / len(split))
        return jnp.repeat(jnp.exp(draws), extent[position] // shards_of).reshape((-1,) + (1,) * (len(extent) - position - 1))

    gain = one(*split[0])
    for cut in split[1:]:
        gain = gain * one(*cut)
    return gain


def centred(own_key, dims, width, bound, cuts=(), held_as=jnp.bfloat16):
    result = width * jax.random.normal(own_key, dims, jnp.float32)
    if cuts:
        result = result * levels(own_key, dims, cuts, -0.22, 0.18)
    return jnp.clip(result, -bound, bound).astype(held_as)


def setup_inputs(seed: int = 0) -> dict:
    key_of = jax.random.split(jax.random.key(seed), 6)
    return {
        "source": centred(key_of[0], (PF, 2, 3, NX, NT, NY * NZ), 1.0, 6.0, ((0, 2), (3, 4), (4, 4)), jnp.float32),
        "links": centred(key_of[1], (4, 2, 3, 3, NX, NT, NY * NZ), 0.35, 2.0, ((0, 2), (4, 4), (5, 4)), jnp.float32),
        "shifts": jnp.clip(jnp.exp(jax.random.uniform(key_of[2], (NSHIFT,), jnp.float32, math.log(0.01), math.log(0.5))), 0.01, 0.5),
        "residues": jnp.clip(jnp.exp(jax.random.uniform(key_of[3], (NSHIFT,), jnp.float32, math.log(0.05), math.log(0.5))), 0.05, 0.5),
        "mass": jnp.clip(jnp.exp(jax.random.uniform(key_of[4], (1,), jnp.float32, math.log(0.1), math.log(0.5))), 0.1, 0.5),
    }


def sign_of(values):
    return (1 - 2 * (values % 2)).astype(jnp.float32)


def phases(coord_x, coord_t, last_t):
    yz_index = jnp.arange(NY * NZ, dtype=jnp.int32)
    ycoord = yz_index // NZ
    zcoord = yz_index % NZ
    unity = jnp.ones((coord_x.shape[0], coord_t.shape[0], NY * NZ), jnp.float32)
    boundary = jnp.where(coord_t == last_t, -1.0, 1.0).astype(jnp.float32)
    eta_y = sign_of(coord_x)[:, None, None] * unity
    eta_z = sign_of(coord_x[:, None, None] + ycoord[None, None, :]) * unity
    eta_t = sign_of(coord_x[:, None, None] + ycoord[None, None, :] + zcoord[None, None, :]) * boundary[None, :, None]
    return jnp.stack([unity, eta_y, eta_z, eta_t])


def times_link(link, field):
    real = jnp.sum(link[0][None] * field[:, 0][:, None] - link[1][None] * field[:, 1][:, None], axis=2)
    imag = jnp.sum(link[0][None] * field[:, 1][:, None] + link[1][None] * field[:, 0][:, None], axis=2)
    return jnp.stack([real, imag], axis=1)


def times_adjoint(link, field):
    real = jnp.sum(link[0][None] * field[:, 0][:, :, None] + link[1][None] * field[:, 1][:, :, None], axis=1)
    imag = jnp.sum(link[0][None] * field[:, 1][:, :, None] - link[1][None] * field[:, 0][:, :, None], axis=1)
    return jnp.stack([real, imag], axis=1)


def roll_ycoord(values, offset):
    return jnp.roll(values, offset * NZ, axis=-1)


def roll_zcoord(values, offset):
    shape = values.shape
    return jnp.roll(values.reshape(shape[:-1] + (NY, NZ)), offset, axis=-1).reshape(shape)


def hopping(field, folded):
    total = times_link(folded[0], jnp.roll(field, -1, axis=3)) - jnp.roll(times_adjoint(folded[0], field), 1, axis=3)
    total = total + times_link(folded[1], roll_ycoord(field, -1)) - roll_ycoord(times_adjoint(folded[1], field), 1)
    total = total + times_link(folded[2], roll_zcoord(field, -1)) - roll_zcoord(times_adjoint(folded[2], field), 1)
    total = total + times_link(folded[3], jnp.roll(field, -1, axis=4)) - jnp.roll(times_adjoint(folded[3], field), 1, axis=4)
    return 0.5 * total


def local_dot(left, right):
    return jnp.sum(left * right, axis=(1, 2, 3, 4, 5))


def spread(values):
    return values.reshape(values.shape + (1, 1, 1, 1, 1))


def rational_of(source, apply_normal, shifts, residues):
    shift_col = shifts[:, None]
    members = source.shape[0]
    residual = source
    direction = source
    solutions = jnp.zeros((shifts.shape[0],) + source.shape, jnp.float32)
    directions = jnp.broadcast_to(source[None], solutions.shape)
    norm_now = local_dot(source, source)
    zeta_now = jnp.ones((shifts.shape[0], members), jnp.float32)
    zeta_old = jnp.ones((shifts.shape[0], members), jnp.float32)
    alpha_old = jnp.ones((members,), jnp.float32)
    beta_old = jnp.zeros((members,), jnp.float32)
    for iteration in range(ITERS):
        image = apply_normal(direction)
        alpha_now = norm_now / local_dot(direction, image)
        zeta_new = zeta_now * zeta_old * alpha_old / (alpha_now * beta_old * (zeta_old - zeta_now) + zeta_old * alpha_old * (1.0 + shift_col * alpha_now))
        alpha_shift = alpha_now * zeta_new / zeta_now
        solutions = solutions + spread(alpha_shift) * directions
        if iteration + 1 < ITERS:
            residual = residual - spread(alpha_now) * image
            norm_next = local_dot(residual, residual)
            beta_now = norm_next / norm_now
            beta_shift = beta_now * (zeta_new / zeta_now) ** 2
            direction = residual + spread(beta_now) * direction
            directions = spread(zeta_new) * residual[None] + spread(beta_shift) * directions
            zeta_old = zeta_now
            zeta_now = zeta_new
            alpha_old = alpha_now
            beta_old = beta_now
            norm_now = norm_next
    return jnp.sum(residues.reshape((-1, 1, 1, 1, 1, 1, 1)) * solutions, axis=0)


def reference(source, links, shifts, residues, mass):
    eta = phases(jnp.arange(NX, dtype=jnp.int32), jnp.arange(NT, dtype=jnp.int32), NT - 1)
    folded = links * eta[:, None, None, None]
    mass_sq = mass[0] * mass[0]

    def apply_normal(field):
        return mass_sq * field - hopping(hopping(field, folded), folded)

    pieces = []
    for member in range(PF):
        pieces.append(rational_of(source[member:member + 1], apply_normal, shifts, residues))
    rational = jnp.concatenate(pieces, axis=0)
    action = (jnp.sum(source * rational) / (PF * NX * NT * NY * NZ)).reshape(1)
    return rational, action
```

```python
import functools

import jax
import jax.numpy as jnp
from jax import lax
from jax.experimental import pallas as pl
from jax.experimental.pallas import tpu as pltpu
from jax.sharding import PartitionSpec as P

NY = 2
NZ = 64
ITERS = 8
PAIRS = 9
MAT = 2 * PAIRS
COMPS = 6


def roll(value, shift, axis):
    size = value.shape[axis]
    return pltpu.roll(value, shift % size, axis)


def kernel(
    dims, source_ref, links_ref, shifts_ref, residues_ref, mass_ref, out_ref, action_ref,
    lk, tfar, xfar, xtwo, sx, sx2, cs_ll, cs_hl, cs_lh, c_ll, c_hl, c_lh,
    gauge, dirn, resid, mid, shiftdirs, rpack, ws, wr, cs, cr, part, act,
    state, lsend, lrecv, hsend, hrecv, psend, precv, asend, arecv,
):
    n_grp, n_zt, n_xy, cells_x, cells_t = dims
    lanes = NY * NZ
    n_all = n_zt * n_xy
    nshift = shifts_ref.shape[0]
    g = lax.axis_index("grp")
    zt = lax.axis_index("zt")
    xy = lax.axis_index("xy")
    me = zt * n_xy + xy
    me_all = g * n_all + me
    x_up, x_dn = lax.rem(xy + 1, n_xy), lax.rem(xy + n_xy - 1, n_xy)
    t_up, t_dn = lax.rem(zt + 1, n_zt), lax.rem(zt + n_zt - 1, n_zt)
    other = 1 - g

    def place(linear):
        inside = lax.rem(linear, n_all)
        return (linear // n_all, inside // n_xy, lax.rem(inside, n_xy))

    def each(count, fn):
        if count <= 32:
            for p in range(1, count):
                fn(p)
        else:
            def step(p, carry):
                fn(p)
                return carry
            lax.fori_loop(1, count, step, 0)

    def copy(src, dst, send, recv, device):
        return pltpu.make_async_remote_copy(
            src_ref=src, dst_ref=dst, send_sem=send, recv_sem=recv,
            device_id=device, device_id_type=pl.DeviceIdType.MESH,
        )

    barrier = pltpu.get_barrier_semaphore()

    def greet(p):
        pl.semaphore_signal(
            barrier, inc=1, device_id=place(lax.rem(me_all + p, n_grp * n_all)),
            device_id_type=pl.DeviceIdType.MESH,
        )

    each(n_grp * n_all, greet)

    sub = lax.broadcasted_iota(jnp.int32, (8, lanes), 0)
    lane = lax.broadcasted_iota(jnp.int32, (8, lanes), 1)
    zcoord = lax.rem(lane, NZ)
    ycoord = lane // NZ
    own = (sub >= 2) & (sub < 2 + cells_t)
    first = sub < cells_t
    late = lax.rem(sub, cells_t) >= 2

    for d in range(2):
        for c in range(MAT):
            low, high = links_ref[c], links_ref[MAT + c]
            if d == 0:
                sx[0, pl.ds(g * MAT + c, 1)] = jnp.where(first, roll(low, 4, 0), high)[None]
            else:
                sx[1, pl.ds(g * MAT + c, 1)] = jnp.where(first, low, roll(high, 4, 0))[None]
    for c in range(2 * MAT):
        lk[pl.ds(g * 2 * MAT + c, 1)] = links_ref[c][None]

    spack = [source_ref[c] for c in range(COMPS)]

    def corner_tiles(tiles, par):
        for k, row in enumerate((7, 4, 3, 0)):
            tile = jnp.zeros((8, lanes), jnp.float32)
            for c in range(COMPS):
                tile = jnp.where(sub == c, jnp.broadcast_to(tiles[c][row:row + 1], (8, lanes)), tile)
            cs[par, k] = tile

    corner_dev = ((g, t_up, x_up), (g, t_dn, x_up), (g, t_up, x_dn), (g, t_dn, x_dn))

    def halo(par):
        routes = ((g, zt, x_up), (g, zt, x_dn), (g, t_up, xy), (g, t_dn, xy))
        found = []
        for k in range(4):
            found.append(copy(cs.at[par, k], cr.at[par, k], hsend.at[par, 4 + k], hrecv.at[par, 4 + k], corner_dev[k]))
        for k in range(4):
            found.append(copy(ws.at[par], wr.at[par, k], hsend.at[par, k], hrecv.at[par, k], routes[k]))
        return found

    def send_part(par):
        def go(p):
            copy(part.at[par, me], part.at[par, me], psend.at[par, p], precv.at[par, me],
                 (g,) + place(lax.rem(me + p, n_all))[1:]).start()
        each(n_all, go)

    def wait_part(par):
        def go(p):
            there = lax.rem(me + n_all - p, n_all)
            done = copy(part.at[par, there], part.at[par, there], psend.at[par, p], precv.at[par, there],
                        (g,) + place(there)[1:])
            done.wait_recv()
            done.wait_send()
        each(n_all, go)

    def dots(rows):
        tile = jnp.zeros((8, lanes), jnp.float32)
        for k, row in enumerate(rows):
            tile = jnp.where(sub == k, jnp.broadcast_to(jnp.sum(row, axis=0, keepdims=True), (8, lanes)), tile)
        return tile

    def summed(ref, par, count):
        if count <= 32:
            total = ref[par, 0]
            for j in range(1, count):
                total = total + ref[par, j]
        else:
            total = lax.fori_loop(1, count, lambda j, acc: acc + ref[par, j], ref[par, 0])
        return jnp.broadcast_to(jnp.sum(total, axis=1, keepdims=True), (8, lanes))

    def fill(values, k):
        return jnp.broadcast_to(values[k:k + 1], (16, lanes))

    def inner(left, right):
        total = left[0] * right[0]
        for c in range(1, COMPS):
            total = total + left[c] * right[c]
        return total

    corner_tiles(spack, 0)
    for c in range(COMPS):
        ws[0, c] = spack[c]
    part[0, pl.ds(me, 1)] = dots([inner(spack, spack)])[None]

    pl.semaphore_wait(barrier, n_grp * n_all - 1)

    half = 2 * MAT
    to_pair = copy(links_ref, lk.at[pl.ds(g * half, half)], lsend.at[0], lrecv.at[0], (other, zt, xy))
    to_pair.start()

    def link_faces(h, src, slot):
        return [
            copy(sx.at[0, pl.ds(h * MAT, MAT)], xfar.at[0, pl.ds(h * MAT, MAT)], lsend.at[slot], lrecv.at[slot], (g, zt, x_up)),
            copy(sx.at[1, pl.ds(h * MAT, MAT)], xfar.at[1, pl.ds(h * MAT, MAT)], lsend.at[slot + 1], lrecv.at[slot + 1], (g, zt, x_dn)),
            copy(src, tfar.at[0, pl.ds(h * half, half)], lsend.at[slot + 2], lrecv.at[slot + 2], (g, t_up, xy)),
            copy(src, tfar.at[1, pl.ds(h * half, half)], lsend.at[slot + 3], lrecv.at[slot + 3], (g, t_dn, xy)),
        ]

    near = link_faces(g, links_ref, 1)
    for item in near:
        item.start()
    send_part(0)
    for item in halo(0):
        item.start()

    to_pair.wait_recv()
    for c in range(MAT):
        low, high = lk[other * half + c], lk[other * half + MAT + c]
        sx[0, pl.ds(other * MAT + c, 1)] = jnp.where(first, roll(low, 4, 0), high)[None]
        sx[1, pl.ds(other * MAT + c, 1)] = jnp.where(first, low, roll(high, 4, 0))[None]
    for c in range(PAIRS):
        sx2[c] = jnp.where(first, lk[c], roll(lk[PAIRS + c], 4, 0))
    for c in range(MAT):
        cs_ll[c:c + 1] = lk[c][7:8]
        cs_ll[MAT + c:MAT + c + 1] = lk[3 * MAT + c][7:8]
        cs_hl[c:c + 1] = lk[3 * MAT + c][3:4]
        cs_lh[c:c + 1] = lk[c][4:5]
    far = link_faces(other, lk.at[pl.ds(other * half, half)], 5) + [
        copy(sx2, xtwo, lsend.at[9], lrecv.at[9], (g, zt, x_up)),
        copy(cs_ll, c_ll, lsend.at[10], lrecv.at[10], corner_dev[0]),
        copy(cs_hl, c_hl, lsend.at[11], lrecv.at[11], corner_dev[2]),
        copy(cs_lh, c_lh, lsend.at[12], lrecv.at[12], corner_dev[1]),
    ]
    for item in far:
        item.start()

    def pick(ref, c):
        return jnp.broadcast_to(ref[c:c + 1], (8, lanes))

    def widen(c, x, mine, low, high):
        between = jnp.where(late, low, high)
        return jnp.where(own, roll(mine, 2 - 4 * x, 0), roll(between, 6 - 4 * x, 0))

    def far_rows(block, low_corner, high_corner, x):
        row = jnp.where(own, roll(block, 2 - 4 * x, 0), 0.0)
        if low_corner is not None:
            row = jnp.where(sub == 1, low_corner, row)
        if high_corner is not None:
            row = jnp.where(sub == 6, high_corner, row)
        return row

    def extend(par, c):
        mine = ws[par, c]
        corner = [jnp.broadcast_to(cr[par, k, c:c + 1], (8, lanes)) for k in range(4)]
        return [
            far_rows(wr[par, 0, c], None, None, 0),
            far_rows(wr[par, 0, c], corner[0], corner[1], 1),
            widen(c, 0, mine, wr[par, 2, c], wr[par, 3, c]),
            widen(c, 1, mine, wr[par, 2, c], wr[par, 3, c]),
            far_rows(wr[par, 1, c], corner[2], corner[3], 0),
            far_rows(wr[par, 1, c], None, None, 1),
        ]

    rows16 = lax.broadcasted_iota(jnp.int32, (16, lanes), 0)
    shift_rows = jnp.zeros((16, lanes), jnp.float32)
    residue_rows = jnp.zeros((16, lanes), jnp.float32)
    for k in range(nshift):
        shift_rows = jnp.where(rows16 == k, shifts_ref[k], shift_rows)
        residue_rows = jnp.where(rows16 == k, residues_ref[k], residue_rows)
    mass_sq = mass_ref[0] * mass_ref[0]

    for c in range(COMPS):
        rpack[c] = spack[c]
        out_ref[c] = jnp.zeros((8, lanes), jnp.float32)
        for k in range(nshift):
            shiftdirs[k, c] = spack[c]

    for item in near + far:
        item.wait()
    to_pair.wait_send()

    t_at = lax.rem(zt * cells_t + sub - 2 + n_zt * cells_t, n_zt * cells_t)
    edge = jnp.where(t_at == n_zt * cells_t - 1, -0.5, 0.5)
    yz_sign = (1 - 2 * lax.rem(ycoord + zcoord, 2)).astype(jnp.float32)
    y_sign = (1 - 2 * lax.rem(ycoord, 2)).astype(jnp.float32)

    def z_up(v):
        cond = jnp.broadcast_to(zcoord == NZ - 1, v.shape)
        return jnp.where(cond, roll(v, NZ - 1, v.ndim - 1), roll(v, -1, v.ndim - 1))

    def z_dn(v):
        cond = jnp.broadcast_to(zcoord == 0, v.shape)
        return jnp.where(cond, roll(v, 1 - NZ, v.ndim - 1), roll(v, 1, v.ndim - 1))

    def wide_link(d, c, e):
        at = d * MAT + c
        sign = -1.0 if e % 2 else 1.0
        if e in (2, 3):
            value = widen(c, e - 2, lk[at], tfar[0, at], tfar[1, at])
        elif e == 0:
            value = far_rows(xtwo[c % PAIRS], None, None, c // PAIRS)
        elif e == 1:
            low = pick(c_ll, c) if d == 0 else (pick(c_ll, MAT + c) if d == 3 else None)
            value = far_rows(xfar[0, (d // 2) * MAT + c], low, pick(c_lh, c) if d == 0 else None, d % 2)
        else:
            value = far_rows(xfar[1, (d // 2) * MAT + c], pick(c_hl, c) if d == 3 else None, None, d % 2)
        if d == 0:
            return 0.5 * value
        if d == 1:
            return (0.5 * sign) * value
        if d == 2:
            return (0.5 * sign) * y_sign * value
        return sign * yz_sign * edge * value

    for part_no in range(2):
        for i in range(3):
            for j in range(3):
                c = part_no * PAIRS + i * 3 + j
                flip = part_no * PAIRS + j * 3 + i
                back = 1.0 if part_no else -1.0
                for e in range(0, 5):
                    wx = wide_link(0, c, e)
                    if e > 0:
                        gauge[0, c, e - 1] = wx
                    if e < 4:
                        gauge[1, flip, e] = back * wx
                for e in range(1, 5):
                    wz = wide_link(2, c, e)
                    gauge[3, c, e - 1] = wz
                    gauge[4, flip, e - 1] = back * z_dn(wz)
                    wt = wide_link(3, c, e)
                    gauge[5, c, e - 1] = wt
                    gauge[6, flip, e - 1] = back * roll(wt, 1, 0)
                    wy = wide_link(1, c, e)
                    turned = wide_link(1, flip, e)
                    gauge[2, c, e - 1] = wy + back * roll(turned, NZ, 1)

    def finish_halo(par):
        for item in halo(par):
            item.wait()

    wait_part(0)
    finish_halo(0)
    for c in range(COMPS):
        wide = extend(0, c)
        for e in range(6):
            dirn[c, e] = wide[e]
            resid[c, e] = wide[e]
    norm = fill(summed(part, 0, n_all), 0)

    def hop(field, e0):
        total = [None] * COMPS
        terms = (
            (0, lambda c: field[c, e0 + 1:e0 + 3]),
            (1, lambda c: field[c, e0 - 1:e0 + 1]),
            (2, lambda c: roll(field[c, e0:e0 + 2], NZ, 2)),
            (3, lambda c: z_up(field[c, e0:e0 + 2])),
            (4, lambda c: z_dn(field[c, e0:e0 + 2])),
            (5, lambda c: roll(field[c, e0:e0 + 2], -1, 1)),
            (6, lambda c: roll(field[c, e0:e0 + 2], 1, 1)),
        )
        for term, shifted in terms:
            v = [shifted(c) for c in range(COMPS)]
            for i in range(3):
                for j in range(3):
                    wre = gauge[term, i * 3 + j, e0 - 1:e0 + 1]
                    wim = gauge[term, PAIRS + i * 3 + j, e0 - 1:e0 + 1]
                    re = wre * v[j] - wim * v[3 + j]
                    im = wre * v[3 + j] + wim * v[j]
                    total[i] = re if total[i] is None else total[i] + re
                    total[3 + i] = im if total[3 + i] is None else total[3 + i] + im
        return total

    def image_of():
        for e0 in (1, 3):
            for c, value in enumerate(hop(dirn, e0)):
                mid[c, e0:e0 + 2] = value
        image = hop(mid, 2)
        packed = []
        dpack = []
        for c in range(COMPS):
            d2, d3 = dirn[c, 2], dirn[c, 3]
            dp = jnp.where(first, roll(d2, -2, 0), roll(d3, 2, 0))
            wp = jnp.where(first, roll(image[c][0], -2, 0), roll(image[c][1], 2, 0))
            dpack.append(dp)
            packed.append(mass_sq * dp - wp)
        return packed, dpack

    def row(values, k):
        return jnp.broadcast_to(values[k:k + 1], (8, lanes))

    def accumulate(gain):
        for c in range(COMPS):
            total = out_ref[c]
            for k in range(nshift):
                total = total + row(gain, k) * shiftdirs[k, c]
            out_ref[c] = total

    def catch_up(gain, zeta_now, beta_shift):
        accumulate(gain)
        for k in range(nshift):
            zk, bk = row(zeta_now, k), row(beta_shift, k)
            for c in range(COMPS):
                shiftdirs[k, c] = zk * rpack[c] + bk * shiftdirs[k, c]

    def iterate(step, last):
        norm, zeta, zeta_old, alpha_old, beta_old, gain, beta_shift = [state[k] for k in range(7)]
        par = step % 2 if last else lax.rem(step, 2)
        packed, dpack = image_of()
        res = [rpack[c] for c in range(COMPS)]
        part[par, pl.ds(me, 1)] = dots([inner(dpack, packed), inner(res, packed), inner(packed, packed)])[None]
        send_part(par)
        if not last:
            corner_tiles(packed, par)
            for c in range(COMPS):
                ws[par, c] = packed[c]
            for item in halo(par):
                item.start()
        catch_up(gain, zeta, beta_shift)
        wait_part(par)
        sums = summed(part, par, n_all)
        alpha = norm / fill(sums, 0)
        zeta_new = zeta * zeta_old * alpha_old / (
            alpha * beta_old * (zeta_old - zeta) + zeta_old * alpha_old * (1.0 + shift_rows * alpha)
        )
        ratio = zeta_new / zeta
        gain = residue_rows * alpha * ratio
        if last:
            return gain
        norm_next = norm - 2.0 * alpha * fill(sums, 1) + alpha * alpha * fill(sums, 2)
        beta = norm_next / norm
        beta_shift = beta * ratio * ratio
        finish_halo(par)
        step_a, step_b = row(alpha, 0), row(beta, 0)
        for c in range(COMPS):
            rpack[c] = rpack[c] - step_a * ws[par, c]
            wide = extend(par, c)
            for e in range(6):
                fresh = resid[c, e] - step_a * wide[e]
                resid[c, e] = fresh
                dirn[c, e] = fresh + step_b * dirn[c, e]
        for k, value in enumerate((norm_next, zeta_new, zeta, alpha, beta, gain, beta_shift)):
            state[k] = value

    one = jnp.ones((16, lanes), jnp.float32)
    none = jnp.zeros((16, lanes), jnp.float32)

    def body(step, carry):
        iterate(step, False)
        return carry

    for k, value in enumerate((norm, one, one, one, none, none, none)):
        state[k] = value
    lax.fori_loop(1, ITERS, body, 0)
    gain = iterate(ITERS, True)
    accumulate(gain)

    answer = [out_ref[c] for c in range(COMPS)]
    act[0, pl.ds(me_all, 1)] = dots([inner(spack, answer)])[None]
    total_devices = n_grp * n_all

    def send_act(p):
        copy(act.at[0, me_all], act.at[0, me_all], asend.at[p], arecv.at[me_all],
             place(lax.rem(me_all + p, total_devices))).start()

    def wait_act(p):
        there = lax.rem(me_all + total_devices - p, total_devices)
        done = copy(act.at[0, there], act.at[0, there], asend.at[p], arecv.at[there], place(there))
        done.wait_recv()
        done.wait_send()

    each(total_devices, send_act)
    each(total_devices, wait_act)
    sites = total_devices * cells_x * cells_t * lanes
    action_ref[...] = summed(act, 0, total_devices) * (1.0 / sites)


def on_device(sizes, source, links, shifts, residues, mass):
    n_grp, n_zt, n_xy = sizes
    cells_x, cells_t, lanes = source.shape[3:]
    n_all = n_zt * n_xy
    f32 = jnp.float32
    tiles = lambda *lead: pltpu.VMEM(lead + (8, lanes), f32)
    rows = lambda count: pltpu.VMEM((count, lanes), f32)
    nshift = shifts.shape[0]
    vmem = pl.BlockSpec(memory_space=pltpu.VMEM)
    smem = pl.BlockSpec(memory_space=pltpu.SMEM)
    dma = pltpu.SemaphoreType.DMA
    rational, action = pl.pallas_call(
        functools.partial(kernel, (n_grp, n_zt, n_xy, cells_x, cells_t)),
        out_shape=(
            jax.ShapeDtypeStruct((COMPS, 8, lanes), f32),
            jax.ShapeDtypeStruct((8, lanes), f32),
        ),
        in_specs=[vmem, vmem, smem, smem, smem],
        out_specs=(vmem, vmem),
        scratch_shapes=[
            tiles(4 * MAT), tiles(2, 4 * MAT), tiles(2, 2 * MAT), tiles(PAIRS), tiles(2, 2 * MAT), tiles(PAIRS),
            rows(40), rows(24), rows(24), rows(40), rows(24), rows(24),
            tiles(7, MAT, 4), tiles(COMPS, 6), tiles(COMPS, 6), tiles(COMPS, 6),
            tiles(nshift, COMPS), tiles(COMPS), tiles(2, COMPS), tiles(2, 4, COMPS),
            tiles(2, 4), tiles(2, 4), tiles(2, n_all), tiles(1, n_grp * n_all),
            pltpu.VMEM((7, 16, lanes), f32),
            dma((13,)), dma((13,)), dma((2, 8)), dma((2, 8)),
            dma((2, n_all)), dma((2, n_all)), dma((n_grp * n_all,)), dma((n_grp * n_all,)),
        ],
        compiler_params=pltpu.CompilerParams(collective_id=0, has_side_effects=True),
    )(
        source.reshape(COMPS, 8, lanes), links.reshape(2 * MAT, 8, lanes), shifts, residues, mass
    )
    return rational.reshape(source.shape), action[0, :1]


def solution(mesh):
    sizes = tuple(mesh.shape[name] for name in ("grp", "zt", "xy"))
    field = P("grp", None, None, "xy", "zt", None)
    return jax.shard_map(
        functools.partial(on_device, sizes),
        mesh=mesh,
        in_specs=(field, P("grp", None, None, None, "xy", "zt", None), P(), P(), P()),
        out_specs=(field, P()),
        check_vma=False,
    )
```

```python
import functools

import jax
import jax.numpy as jnp
from jax import lax
from jax.experimental import pallas as pl
from jax.experimental.pallas import tpu as pltpu
from jax.sharding import PartitionSpec as P

NY = 2
NZ = 64
ITERS = 8
PAIRS = 9
MAT = 2 * PAIRS
COMPS = 6


def roll(value, shift, axis):
    size = value.shape[axis]
    return pltpu.roll(value, shift % size, axis)


def kernel(
    dims, source_ref, links_ref, shifts_ref, residues_ref, mass_ref, out_ref, action_ref,
    lk, tfar, xfar, xtwo, sx, sx2, cs_ll, cs_hl, cs_lh, c_ll, c_hl, c_lh,
    gauge, dirn, resid, mid, shiftdirs, rpack, ws, wr, cs, cr, part, act,
    state, lsend, lrecv, hsend, hrecv, psend, precv, asend, arecv,
):
    n_grp, n_zt, n_xy, cells_x, cells_t = dims
    lanes = NY * NZ
    n_all = n_zt * n_xy
    nshift = shifts_ref.shape[0]
    g = lax.axis_index("grp")
    zt = lax.axis_index("zt")
    xy = lax.axis_index("xy")
    me = zt * n_xy + xy
    me_all = g * n_all + me
    x_up, x_dn = lax.rem(xy + 1, n_xy), lax.rem(xy + n_xy - 1, n_xy)
    t_up, t_dn = lax.rem(zt + 1, n_zt), lax.rem(zt + n_zt - 1, n_zt)
    other = 1 - g

    def place(linear):
        inside = lax.rem(linear, n_all)
        return (linear // n_all, inside // n_xy, lax.rem(inside, n_xy))

    def each(count, fn):
        if count <= 32:
            for p in range(1, count):
                fn(p)
        else:
            def step(p, carry):
                fn(p)
                return carry
            lax.fori_loop(1, count, step, 0)

    def copy(src, dst, send, recv, device):
        return pltpu.make_async_remote_copy(
            src_ref=src, dst_ref=dst, send_sem=send, recv_sem=recv,
            device_id=device, device_id_type=pl.DeviceIdType.MESH,
        )

    barrier = pltpu.get_barrier_semaphore()

    def greet(p):
        pl.semaphore_signal(
            barrier, inc=1, device_id=place(lax.rem(me_all + p, n_grp * n_all)),
            device_id_type=pl.DeviceIdType.MESH,
        )

    each(n_grp * n_all, greet)

    sub = lax.broadcasted_iota(jnp.int32, (8, lanes), 0)
    lane = lax.broadcasted_iota(jnp.int32, (8, lanes), 1)
    zcoord = lax.rem(lane, NZ)
    ycoord = lane // NZ
    quarter = lanes // 4
    home = sub == lane // quarter
    own = (sub >= 2) & (sub < 2 + cells_t)
    first = sub < cells_t
    late = lax.rem(sub, cells_t) >= 2

    for d in range(2):
        for c in range(MAT):
            low, high = links_ref[c], links_ref[MAT + c]
            if d == 0:
                sx[0, pl.ds(g * MAT + c, 1)] = jnp.where(first, roll(low, 4, 0), high)[None]
            else:
                sx[1, pl.ds(g * MAT + c, 1)] = jnp.where(first, low, roll(high, 4, 0))[None]
    for c in range(2 * MAT):
        lk[pl.ds(g * 2 * MAT + c, 1)] = links_ref[c][None]

    spack = [source_ref[c] for c in range(COMPS)]

    def corner_tiles(tiles, par):
        for k, row in enumerate((7, 4, 3, 0)):
            tile = jnp.zeros((8, lanes), jnp.float32)
            for c in range(COMPS):
                tile = jnp.where(sub == c, jnp.broadcast_to(tiles[c][row:row + 1], (8, lanes)), tile)
            cs[par, k] = tile

    corner_dev = ((g, t_up, x_up), (g, t_dn, x_up), (g, t_up, x_dn), (g, t_dn, x_dn))

    def halo(par):
        routes = ((g, zt, x_up), (g, zt, x_dn), (g, t_up, xy), (g, t_dn, xy))
        found = []
        for k in range(4):
            found.append(copy(cs.at[par, k], cr.at[par, k], hsend.at[par, 4 + k], hrecv.at[par, 4 + k], corner_dev[k]))
        for k in range(4):
            found.append(copy(ws.at[par], wr.at[par, k], hsend.at[par, k], hrecv.at[par, k], routes[k]))
        return found

    def send_part(par):
        def go(p):
            copy(part.at[par, me], part.at[par, me], psend.at[par, p], precv.at[par, me],
                 (g,) + place(lax.rem(me + p, n_all))[1:]).start()
        each(n_all, go)

    def wait_part(par):
        def go(p):
            there = lax.rem(me + n_all - p, n_all)
            done = copy(part.at[par, there], part.at[par, there], psend.at[par, p], precv.at[par, there],
                        (g,) + place(there)[1:])
            done.wait_recv()
            done.wait_send()
        each(n_all, go)

    def dots(rows):
        tile = jnp.zeros((8, lanes), jnp.float32)
        for k, row in enumerate(rows):
            tile = jnp.where(sub == k, jnp.broadcast_to(jnp.sum(row, axis=0, keepdims=True), (8, lanes)), tile)
        tile = tile + roll(tile, 2 * quarter, 1)
        tile = tile + roll(tile, quarter, 1)
        return jnp.sum(jnp.where(home, tile, 0.0), axis=0, keepdims=True)

    def summed(par):
        if n_all <= 32:
            level = [part[par, j] for j in range(n_all)]
            while len(level) > 1:
                odd = level[len(level) // 2 * 2:]
                level = [level[k] + level[k + 1] for k in range(0, len(level) - 1, 2)] + odd
            total = level[0]
        else:
            total = lax.fori_loop(1, n_all, lambda j, acc: acc + part[par, j], part[par, 0])
        split = jnp.where(home, jnp.broadcast_to(total, (8, lanes)), 0.0)
        return jnp.broadcast_to(jnp.sum(split, axis=1, keepdims=True), (8, lanes))

    def fill(values, k):
        return jnp.broadcast_to(values[k:k + 1], (16, lanes))

    def inner(left, right):
        total = left[0] * right[0]
        for c in range(1, COMPS):
            total = total + left[c] * right[c]
        return total

    corner_tiles(spack, 0)
    for c in range(COMPS):
        ws[0, c] = spack[c]
    part[0, pl.ds(me, 1)] = dots([inner(spack, spack)])[None]

    pl.semaphore_wait(barrier, n_grp * n_all - 1)

    half = 2 * MAT
    to_pair = copy(links_ref, lk.at[pl.ds(g * half, half)], lsend.at[0], lrecv.at[0], (other, zt, xy))
    to_pair.start()

    def link_faces(h, src, slot):
        return [
            copy(sx.at[0, pl.ds(h * MAT, MAT)], xfar.at[0, pl.ds(h * MAT, MAT)], lsend.at[slot], lrecv.at[slot], (g, zt, x_up)),
            copy(sx.at[1, pl.ds(h * MAT, MAT)], xfar.at[1, pl.ds(h * MAT, MAT)], lsend.at[slot + 1], lrecv.at[slot + 1], (g, zt, x_dn)),
            copy(src, tfar.at[0, pl.ds(h * half, half)], lsend.at[slot + 2], lrecv.at[slot + 2], (g, t_up, xy)),
            copy(src, tfar.at[1, pl.ds(h * half, half)], lsend.at[slot + 3], lrecv.at[slot + 3], (g, t_dn, xy)),
        ]

    near = link_faces(g, links_ref, 1)
    for item in near:
        item.start()
    send_part(0)
    for item in halo(0):
        item.start()

    to_pair.wait_recv()
    for c in range(MAT):
        low, high = lk[other * half + c], lk[other * half + MAT + c]
        sx[0, pl.ds(other * MAT + c, 1)] = jnp.where(first, roll(low, 4, 0), high)[None]
        sx[1, pl.ds(other * MAT + c, 1)] = jnp.where(first, low, roll(high, 4, 0))[None]
    for c in range(PAIRS):
        sx2[c] = jnp.where(first, lk[c], roll(lk[PAIRS + c], 4, 0))
    for c in range(MAT):
        cs_ll[c:c + 1] = lk[c][7:8]
        cs_ll[MAT + c:MAT + c + 1] = lk[3 * MAT + c][7:8]
        cs_hl[c:c + 1] = lk[3 * MAT + c][3:4]
        cs_lh[c:c + 1] = lk[c][4:5]
    far = link_faces(other, lk.at[pl.ds(other * half, half)], 5) + [
        copy(sx2, xtwo, lsend.at[9], lrecv.at[9], (g, zt, x_up)),
        copy(cs_ll, c_ll, lsend.at[10], lrecv.at[10], corner_dev[0]),
        copy(cs_hl, c_hl, lsend.at[11], lrecv.at[11], corner_dev[2]),
        copy(cs_lh, c_lh, lsend.at[12], lrecv.at[12], corner_dev[1]),
    ]
    for item in far:
        item.start()

    def pick(ref, c):
        return jnp.broadcast_to(ref[c:c + 1], (8, lanes))

    def widen(c, x, mine, low, high):
        between = jnp.where(late, low, high)
        return jnp.where(own, roll(mine, 2 - 4 * x, 0), roll(between, 6 - 4 * x, 0))

    def far_rows(block, low_corner, high_corner, x):
        row = jnp.where(own, roll(block, 2 - 4 * x, 0), 0.0)
        if low_corner is not None:
            row = jnp.where(sub == 1, low_corner, row)
        if high_corner is not None:
            row = jnp.where(sub == 6, high_corner, row)
        return row

    def extend(par, c):
        mine = ws[par, c]
        corner = [jnp.broadcast_to(cr[par, k, c:c + 1], (8, lanes)) for k in range(4)]
        return [
            far_rows(wr[par, 0, c], None, None, 0),
            far_rows(wr[par, 0, c], corner[0], corner[1], 1),
            widen(c, 0, mine, wr[par, 2, c], wr[par, 3, c]),
            widen(c, 1, mine, wr[par, 2, c], wr[par, 3, c]),
            far_rows(wr[par, 1, c], corner[2], corner[3], 0),
            far_rows(wr[par, 1, c], None, None, 1),
        ]

    rows16 = lax.broadcasted_iota(jnp.int32, (16, lanes), 0)
    shift_rows = jnp.zeros((16, lanes), jnp.float32)
    residue_rows = jnp.zeros((16, lanes), jnp.float32)
    for k in range(nshift):
        shift_rows = jnp.where(rows16 == k, shifts_ref[k], shift_rows)
        residue_rows = jnp.where(rows16 == k, residues_ref[k], residue_rows)
    mass_sq = mass_ref[0] * mass_ref[0]

    for c in range(COMPS):
        rpack[c] = spack[c]
        out_ref[c] = jnp.zeros((8, lanes), jnp.float32)
        for k in range(nshift):
            shiftdirs[k, c] = spack[c]

    for item in near[2:] + far[2:4]:
        item.wait()
    to_pair.wait_send()

    t_at = lax.rem(zt * cells_t + sub - 2 + n_zt * cells_t, n_zt * cells_t)
    edge = jnp.where(t_at == n_zt * cells_t - 1, -0.5, 0.5)
    yz_sign = (1 - 2 * lax.rem(ycoord + zcoord, 2)).astype(jnp.float32)
    y_sign = (1 - 2 * lax.rem(ycoord, 2)).astype(jnp.float32)

    def z_up(v):
        cond = jnp.broadcast_to(zcoord == NZ - 1, v.shape)
        return jnp.where(cond, roll(v, NZ - 1, v.ndim - 1), roll(v, -1, v.ndim - 1))

    def z_dn(v):
        cond = jnp.broadcast_to(zcoord == 0, v.shape)
        return jnp.where(cond, roll(v, 1 - NZ, v.ndim - 1), roll(v, 1, v.ndim - 1))

    def wide_link(d, c, e):
        at = d * MAT + c
        sign = -1.0 if e % 2 else 1.0
        if e in (2, 3):
            value = widen(c, e - 2, lk[at], tfar[0, at], tfar[1, at])
        elif e == 0:
            value = far_rows(xtwo[c % PAIRS], None, None, c // PAIRS)
        elif e == 1:
            low = pick(c_ll, c) if d == 0 else (pick(c_ll, MAT + c) if d == 3 else None)
            value = far_rows(xfar[0, (d // 2) * MAT + c], low, pick(c_lh, c) if d == 0 else None, d % 2)
        else:
            value = far_rows(xfar[1, (d // 2) * MAT + c], pick(c_hl, c) if d == 3 else None, None, d % 2)
        if d == 0:
            return 0.5 * value
        if d == 1:
            return (0.5 * sign) * value
        if d == 2:
            return (0.5 * sign) * y_sign * value
        return sign * yz_sign * edge * value

    def build(rows):
        for part_no in range(2):
            for i in range(3):
                for j in range(3):
                    c = part_no * PAIRS + i * 3 + j
                    flip = part_no * PAIRS + j * 3 + i
                    back = 1.0 if part_no else -1.0
                    for e in rows:
                        wx = wide_link(0, c, e)
                        if e > 0:
                            gauge[0, c, e - 1] = wx
                        if e < 4:
                            gauge[1, flip, e] = back * wx
                        if e == 0:
                            continue
                        wz = wide_link(2, c, e)
                        gauge[3, c, e - 1] = wz
                        gauge[4, flip, e - 1] = back * z_dn(wz)
                        wt = wide_link(3, c, e)
                        gauge[5, c, e - 1] = wt
                        gauge[6, flip, e - 1] = back * roll(wt, 1, 0)
                        wy = wide_link(1, c, e)
                        turned = wide_link(1, flip, e)
                        gauge[2, c, e - 1] = wy + back * roll(turned, NZ, 1)

    build((2, 3))
    for item in near[:2] + far[:2] + far[4:]:
        item.wait()
    build((0, 1, 4))

    def finish_halo(par):
        for item in halo(par):
            item.wait()

    wait_part(0)
    finish_halo(0)
    for c in range(COMPS):
        wide = extend(0, c)
        for e in range(6):
            dirn[c, e] = wide[e]
            resid[c, e] = wide[e]
    norm = fill(summed(0), 0)

    def hop(field, e0):
        total = [None] * COMPS
        terms = (
            (0, lambda c: field[c, e0 + 1:e0 + 3]),
            (1, lambda c: field[c, e0 - 1:e0 + 1]),
            (2, lambda c: roll(field[c, e0:e0 + 2], NZ, 2)),
            (3, lambda c: z_up(field[c, e0:e0 + 2])),
            (4, lambda c: z_dn(field[c, e0:e0 + 2])),
            (5, lambda c: roll(field[c, e0:e0 + 2], -1, 1)),
            (6, lambda c: roll(field[c, e0:e0 + 2], 1, 1)),
        )
        for term, shifted in terms:
            v = [shifted(c) for c in range(COMPS)]
            for i in range(3):
                for j in range(3):
                    wre = gauge[term, i * 3 + j, e0 - 1:e0 + 1]
                    wim = gauge[term, PAIRS + i * 3 + j, e0 - 1:e0 + 1]
                    re = wre * v[j] - wim * v[3 + j]
                    im = wre * v[3 + j] + wim * v[j]
                    total[i] = re if total[i] is None else total[i] + re
                    total[3 + i] = im if total[3 + i] is None else total[3 + i] + im
        return total

    def image_of():
        for e0 in (1, 3):
            for c, value in enumerate(hop(dirn, e0)):
                mid[c, e0:e0 + 2] = value
        image = hop(mid, 2)
        packed = []
        dpack = []
        for c in range(COMPS):
            d2, d3 = dirn[c, 2], dirn[c, 3]
            dp = jnp.where(first, roll(d2, -2, 0), roll(d3, 2, 0))
            wp = jnp.where(first, roll(image[c][0], -2, 0), roll(image[c][1], 2, 0))
            dpack.append(dp)
            packed.append(mass_sq * dp - wp)
        return packed, dpack

    def row(values, k):
        return jnp.broadcast_to(values[k:k + 1], (8, lanes))

    def accumulate(gain):
        for c in range(COMPS):
            total = out_ref[c]
            for k in range(nshift):
                total = total + row(gain, k) * shiftdirs[k, c]
            out_ref[c] = total

    def catch_up(gain, zeta_now, beta_shift):
        accumulate(gain)
        for k in range(nshift):
            zk, bk = row(zeta_now, k), row(beta_shift, k)
            for c in range(COMPS):
                shiftdirs[k, c] = zk * rpack[c] + bk * shiftdirs[k, c]

    def iterate(step, last):
        norm, zeta, zeta_old, alpha_old, beta_old, gain, beta_shift, along, score = [state[k] for k in range(9)]
        par = step % 2 if last else lax.rem(step, 2)
        packed, dpack = image_of()
        res = [rpack[c] for c in range(COMPS)]
        part[par, pl.ds(me, 1)] = dots([inner(dpack, packed), inner(res, packed), inner(packed, packed), inner(spack, res)])[None]
        send_part(par)
        if not last:
            corner_tiles(packed, par)
            for c in range(COMPS):
                ws[par, c] = packed[c]
            for item in halo(par):
                item.start()
        catch_up(gain, zeta, beta_shift)
        wait_part(par)
        sums = summed(par)
        alpha = norm / fill(sums, 0)
        zeta_new = zeta * zeta_old * alpha_old / (
            alpha * beta_old * (zeta_old - zeta) + zeta_old * alpha_old * (1.0 + shift_rows * alpha)
        )
        ratio = zeta_new / zeta
        along = zeta * fill(sums, 3) + beta_shift * along
        gain = residue_rows * alpha * ratio
        score = score + gain * along
        if last:
            return gain, score
        norm_next = norm - 2.0 * alpha * fill(sums, 1) + alpha * alpha * fill(sums, 2)
        beta = norm_next / norm
        beta_shift = beta * ratio * ratio
        finish_halo(par)
        step_a, step_b = row(alpha, 0), row(beta, 0)
        for c in range(COMPS):
            rpack[c] = rpack[c] - step_a * ws[par, c]
            wide = extend(par, c)
            for e in range(6):
                fresh = resid[c, e] - step_a * wide[e]
                resid[c, e] = fresh
                dirn[c, e] = fresh + step_b * dirn[c, e]
        for k, value in enumerate((norm_next, zeta_new, zeta, alpha, beta, gain, beta_shift, along, score)):
            state[k] = value

    one = jnp.ones((16, lanes), jnp.float32)
    none = jnp.zeros((16, lanes), jnp.float32)

    def body(step, carry):
        iterate(step, False)
        return carry

    for k, value in enumerate((norm, one, one, one, none, none, none, none, none)):
        state[k] = value
    lax.fori_loop(1, ITERS, body, 0)
    gain, score = iterate(ITERS, True)
    act[g] = jnp.sum(score, axis=0, keepdims=True)

    def swap(p):
        device = (lax.rem(g + p, n_grp), zt, xy)
        return copy(act.at[g], act.at[g], asend.at[p], arecv.at[g], device)

    def swapped(p):
        there = lax.rem(g + n_grp - p, n_grp)
        return copy(act.at[there], act.at[there], asend.at[p], arecv.at[there], (there, zt, xy))

    for p in range(1, n_grp):
        swap(p).start()
    accumulate(gain)
    for p in range(1, n_grp):
        swapped(p).wait_recv()
        swap(p).wait_send()
    total = act[0]
    for k in range(1, n_grp):
        total = total + act[k]
    sites = n_grp * n_all * cells_x * cells_t * lanes
    action_ref[0] = jnp.max(total) * (1.0 / sites)


def on_device(sizes, source, links, shifts, residues, mass):
    n_grp, n_zt, n_xy = sizes
    cells_x, cells_t, lanes = source.shape[3:]
    n_all = n_zt * n_xy
    f32 = jnp.float32
    tiles = lambda *lead: pltpu.VMEM(lead + (8, lanes), f32)
    rows = lambda count: pltpu.VMEM((count, lanes), f32)
    nshift = shifts.shape[0]
    vmem = pl.BlockSpec(memory_space=pltpu.VMEM)
    smem = pl.BlockSpec(memory_space=pltpu.SMEM)
    dma = pltpu.SemaphoreType.DMA
    rational, action = pl.pallas_call(
        functools.partial(kernel, (n_grp, n_zt, n_xy, cells_x, cells_t)),
        out_shape=(
            jax.ShapeDtypeStruct((COMPS, 8, lanes), f32),
            jax.ShapeDtypeStruct((1,), f32),
        ),
        in_specs=[vmem, vmem, smem, smem, smem],
        out_specs=(vmem, smem),
        scratch_shapes=[
            tiles(4 * MAT), tiles(2, 4 * MAT), tiles(2, 2 * MAT), tiles(PAIRS), tiles(2, 2 * MAT), tiles(PAIRS),
            rows(40), rows(24), rows(24), rows(40), rows(24), rows(24),
            tiles(7, MAT, 4), tiles(COMPS, 6), tiles(COMPS, 6), tiles(COMPS, 6),
            tiles(nshift, COMPS), tiles(COMPS), tiles(2, COMPS), tiles(2, 4, COMPS),
            tiles(2, 4), tiles(2, 4), pltpu.VMEM((2, n_all, 1, lanes), f32), pltpu.VMEM((n_grp, 1, lanes), f32),
            pltpu.VMEM((9, 16, lanes), f32),
            dma((13,)), dma((13,)), dma((2, 8)), dma((2, 8)),
            dma((2, n_all)), dma((2, n_all)), dma((n_grp,)), dma((n_grp,)),
        ],
        compiler_params=pltpu.CompilerParams(collective_id=0, has_side_effects=True),
    )(
        source.reshape(COMPS, 8, lanes), links.reshape(2 * MAT, 8, lanes), shifts, residues, mass
    )
    return rational.reshape(source.shape), action


def solution(mesh):
    sizes = tuple(mesh.shape[name] for name in ("grp", "zt", "xy"))
    field = P("grp", None, None, "xy", "zt", None)
    return jax.shard_map(
        functools.partial(on_device, sizes),
        mesh=mesh,
        in_specs=(field, P("grp", None, None, None, "xy", "zt", None), P(), P(), P()),
        out_specs=(field, P()),
        check_vma=False,
    )
```

```python
import functools

import jax
import jax.numpy as jnp
from jax import lax
from jax.experimental import pallas as pl
from jax.experimental.pallas import tpu as pltpu
from jax.sharding import PartitionSpec as P

NY = 2
NZ = 64
ITERS = 8
PAIRS = 9
MAT = 2 * PAIRS
COMPS = 6


def roll(value, shift, axis):
    size = value.shape[axis]
    return pltpu.roll(value, shift % size, axis)


def kernel(
    dims, source_hbm, links_hbm, shifts_ref, residues_ref, mass_ref, out_ref, action_ref,
    lk, tfar, xfar, xtwo, sx, sx2, cs_ll, cs_hl, cs_lh, c_ll, c_hl, c_lh,
    gauge, dirn, resid, mid, shiftdirs, rpack, ws, wr, cs, cr, part, act,
    state, source_ref, links_ref, isem, lsend, lrecv, hsend, hrecv, psend, precv, asend, arecv,
):
    n_grp, n_zt, n_xy, cells_x, cells_t = dims
    lanes = NY * NZ
    n_all = n_zt * n_xy
    nshift = shifts_ref.shape[0]
    g = lax.axis_index("grp")
    zt = lax.axis_index("zt")
    xy = lax.axis_index("xy")
    me = zt * n_xy + xy
    me_all = g * n_all + me
    x_up, x_dn = lax.rem(xy + 1, n_xy), lax.rem(xy + n_xy - 1, n_xy)
    t_up, t_dn = lax.rem(zt + 1, n_zt), lax.rem(zt + n_zt - 1, n_zt)
    other = 1 - g

    def place(linear):
        inside = lax.rem(linear, n_all)
        return (linear // n_all, inside // n_xy, lax.rem(inside, n_xy))

    def each(count, fn):
        if count <= 32:
            for p in range(1, count):
                fn(p)
        else:
            def step(p, carry):
                fn(p)
                return carry
            lax.fori_loop(1, count, step, 0)

    def copy(src, dst, send, recv, device):
        return pltpu.make_async_remote_copy(
            src_ref=src, dst_ref=dst, send_sem=send, recv_sem=recv,
            device_id=device, device_id_type=pl.DeviceIdType.MESH,
        )

    barrier = pltpu.get_barrier_semaphore()

    def greet(p):
        pl.semaphore_signal(
            barrier, inc=1, device_id=place(lax.rem(me_all + p, n_grp * n_all)),
            device_id_type=pl.DeviceIdType.MESH,
        )

    fetch_links = pltpu.make_async_copy(links_hbm, links_ref, isem.at[0])
    fetch_source = pltpu.make_async_copy(source_hbm, source_ref, isem.at[1])
    fetch_links.start()
    fetch_source.start()
    each(n_grp * n_all, greet)
    fetch_links.wait()
    fetch_source.wait()

    sub = lax.broadcasted_iota(jnp.int32, (8, lanes), 0)
    lane = lax.broadcasted_iota(jnp.int32, (8, lanes), 1)
    zcoord = lax.rem(lane, NZ)
    ycoord = lane // NZ
    quarter = lanes // 4
    home = sub == lane // quarter
    own = (sub >= 2) & (sub < 2 + cells_t)
    first = sub < cells_t
    late = lax.rem(sub, cells_t) >= 2

    for d in range(2):
        for c in range(MAT):
            low, high = links_ref[c], links_ref[MAT + c]
            if d == 0:
                sx[0, pl.ds(g * MAT + c, 1)] = jnp.where(first, roll(low, 4, 0), high)[None]
            else:
                sx[1, pl.ds(g * MAT + c, 1)] = jnp.where(first, low, roll(high, 4, 0))[None]
    for c in range(2 * MAT):
        lk[pl.ds(g * 2 * MAT + c, 1)] = links_ref[c][None]

    spack = [source_ref[c] for c in range(COMPS)]

    def corner_tiles(tiles, par):
        for k, row in enumerate((7, 4, 3, 0)):
            tile = jnp.zeros((8, lanes), jnp.float32)
            for c in range(COMPS):
                tile = jnp.where(sub == c, jnp.broadcast_to(tiles[c][row:row + 1], (8, lanes)), tile)
            cs[par, k] = tile

    corner_dev = ((g, t_up, x_up), (g, t_dn, x_up), (g, t_up, x_dn), (g, t_dn, x_dn))

    def halo(par):
        routes = ((g, zt, x_up), (g, zt, x_dn), (g, t_up, xy), (g, t_dn, xy))
        found = []
        for k in range(4):
            found.append(copy(cs.at[par, k], cr.at[par, k], hsend.at[par, 4 + k], hrecv.at[par, 4 + k], corner_dev[k]))
        for k in range(4):
            found.append(copy(ws.at[par], wr.at[par, k], hsend.at[par, k], hrecv.at[par, k], routes[k]))
        return found

    def send_part(par):
        def go(p):
            copy(part.at[par, me], part.at[par, me], psend.at[par, p], precv.at[par, me],
                 (g,) + place(lax.rem(me + p, n_all))[1:]).start()
        each(n_all, go)

    def wait_part(par):
        def go(p):
            there = lax.rem(me + n_all - p, n_all)
            done = copy(part.at[par, there], part.at[par, there], psend.at[par, p], precv.at[par, there],
                        (g,) + place(there)[1:])
            done.wait_recv()
            done.wait_send()
        each(n_all, go)

    def dots(rows):
        tile = jnp.zeros((8, lanes), jnp.float32)
        for k, row in enumerate(rows):
            tile = jnp.where(sub == k, jnp.broadcast_to(jnp.sum(row, axis=0, keepdims=True), (8, lanes)), tile)
        tile = tile + roll(tile, 2 * quarter, 1)
        tile = tile + roll(tile, quarter, 1)
        return jnp.sum(jnp.where(home, tile, 0.0), axis=0, keepdims=True)

    def summed(par):
        if n_all <= 32:
            level = [part[par, j] for j in range(n_all)]
            while len(level) > 1:
                odd = level[len(level) // 2 * 2:]
                level = [level[k] + level[k + 1] for k in range(0, len(level) - 1, 2)] + odd
            total = level[0]
        else:
            total = lax.fori_loop(1, n_all, lambda j, acc: acc + part[par, j], part[par, 0])
        split = jnp.where(home, jnp.broadcast_to(total, (8, lanes)), 0.0)
        return jnp.broadcast_to(jnp.sum(split, axis=1, keepdims=True), (8, lanes))

    def fill(values, k):
        return jnp.broadcast_to(values[k:k + 1], (16, lanes))

    def inner(left, right):
        total = left[0] * right[0]
        for c in range(1, COMPS):
            total = total + left[c] * right[c]
        return total

    corner_tiles(spack, 0)
    for c in range(COMPS):
        ws[0, c] = spack[c]
    part[0, pl.ds(me, 1)] = dots([inner(spack, spack)])[None]

    pl.semaphore_wait(barrier, n_grp * n_all - 1)

    half = 2 * MAT
    to_pair = copy(links_ref, lk.at[pl.ds(g * half, half)], lsend.at[0], lrecv.at[0], (other, zt, xy))
    to_pair.start()

    def link_faces(h, src, slot):
        return [
            copy(sx.at[0, pl.ds(h * MAT, MAT)], xfar.at[0, pl.ds(h * MAT, MAT)], lsend.at[slot], lrecv.at[slot], (g, zt, x_up)),
            copy(sx.at[1, pl.ds(h * MAT, MAT)], xfar.at[1, pl.ds(h * MAT, MAT)], lsend.at[slot + 1], lrecv.at[slot + 1], (g, zt, x_dn)),
            copy(src, tfar.at[0, pl.ds(h * half, half)], lsend.at[slot + 2], lrecv.at[slot + 2], (g, t_up, xy)),
            copy(src, tfar.at[1, pl.ds(h * half, half)], lsend.at[slot + 3], lrecv.at[slot + 3], (g, t_dn, xy)),
        ]

    near = link_faces(g, links_ref, 1)
    for item in near:
        item.start()
    send_part(0)
    for item in halo(0):
        item.start()

    to_pair.wait_recv()
    for c in range(MAT):
        low, high = lk[other * half + c], lk[other * half + MAT + c]
        sx[0, pl.ds(other * MAT + c, 1)] = jnp.where(first, roll(low, 4, 0), high)[None]
        sx[1, pl.ds(other * MAT + c, 1)] = jnp.where(first, low, roll(high, 4, 0))[None]
    for c in range(PAIRS):
        sx2[c] = jnp.where(first, lk[c], roll(lk[PAIRS + c], 4, 0))
    for c in range(MAT):
        cs_ll[c:c + 1] = lk[c][7:8]
        cs_ll[MAT + c:MAT + c + 1] = lk[3 * MAT + c][7:8]
        cs_hl[c:c + 1] = lk[3 * MAT + c][3:4]
        cs_lh[c:c + 1] = lk[c][4:5]
    far = link_faces(other, lk.at[pl.ds(other * half, half)], 5) + [
        copy(sx2, xtwo, lsend.at[9], lrecv.at[9], (g, zt, x_up)),
        copy(cs_ll, c_ll, lsend.at[10], lrecv.at[10], corner_dev[0]),
        copy(cs_hl, c_hl, lsend.at[11], lrecv.at[11], corner_dev[2]),
        copy(cs_lh, c_lh, lsend.at[12], lrecv.at[12], corner_dev[1]),
    ]
    for item in far:
        item.start()

    def pick(ref, c):
        return jnp.broadcast_to(ref[c:c + 1], (8, lanes))

    def widen(c, x, mine, low, high):
        between = jnp.where(late, low, high)
        return jnp.where(own, roll(mine, 2 - 4 * x, 0), roll(between, 6 - 4 * x, 0))

    def far_rows(block, low_corner, high_corner, x):
        row = jnp.where(own, roll(block, 2 - 4 * x, 0), 0.0)
        if low_corner is not None:
            row = jnp.where(sub == 1, low_corner, row)
        if high_corner is not None:
            row = jnp.where(sub == 6, high_corner, row)
        return row

    def extend(par, c):
        mine = ws[par, c]
        corner = [jnp.broadcast_to(cr[par, k, c:c + 1], (8, lanes)) for k in range(4)]
        return [
            far_rows(wr[par, 0, c], None, None, 0),
            far_rows(wr[par, 0, c], corner[0], corner[1], 1),
            widen(c, 0, mine, wr[par, 2, c], wr[par, 3, c]),
            widen(c, 1, mine, wr[par, 2, c], wr[par, 3, c]),
            far_rows(wr[par, 1, c], corner[2], corner[3], 0),
            far_rows(wr[par, 1, c], None, None, 1),
        ]

    rows16 = lax.broadcasted_iota(jnp.int32, (16, lanes), 0)
    shift_rows = jnp.zeros((16, lanes), jnp.float32)
    residue_rows = jnp.zeros((16, lanes), jnp.float32)
    for k in range(nshift):
        shift_rows = jnp.where(rows16 == k, shifts_ref[k], shift_rows)
        residue_rows = jnp.where(rows16 == k, residues_ref[k], residue_rows)
    mass_sq = mass_ref[0] * mass_ref[0]

    for c in range(COMPS):
        rpack[c] = spack[c]
        out_ref[c] = jnp.zeros((8, lanes), jnp.float32)
        for k in range(nshift):
            shiftdirs[k, c] = spack[c]

    for item in near[2:] + far[2:4]:
        item.wait()
    to_pair.wait_send()

    t_at = lax.rem(zt * cells_t + sub - 2 + n_zt * cells_t, n_zt * cells_t)
    edge = jnp.where(t_at == n_zt * cells_t - 1, -0.5, 0.5)
    yz_sign = (1 - 2 * lax.rem(ycoord + zcoord, 2)).astype(jnp.float32)
    y_sign = (1 - 2 * lax.rem(ycoord, 2)).astype(jnp.float32)

    def z_up(v):
        cond = jnp.broadcast_to(zcoord == NZ - 1, v.shape)
        return jnp.where(cond, roll(v, NZ - 1, v.ndim - 1), roll(v, -1, v.ndim - 1))

    def z_dn(v):
        cond = jnp.broadcast_to(zcoord == 0, v.shape)
        return jnp.where(cond, roll(v, 1 - NZ, v.ndim - 1), roll(v, 1, v.ndim - 1))

    def wide_link(d, c, e):
        at = d * MAT + c
        sign = -1.0 if e % 2 else 1.0
        if e in (2, 3):
            value = widen(c, e - 2, lk[at], tfar[0, at], tfar[1, at])
        elif e == 0:
            value = far_rows(xtwo[c % PAIRS], None, None, c // PAIRS)
        elif e == 1:
            low = pick(c_ll, c) if d == 0 else (pick(c_ll, MAT + c) if d == 3 else None)
            value = far_rows(xfar[0, (d // 2) * MAT + c], low, pick(c_lh, c) if d == 0 else None, d % 2)
        else:
            value = far_rows(xfar[1, (d // 2) * MAT + c], pick(c_hl, c) if d == 3 else None, None, d % 2)
        if d == 0:
            return 0.5 * value
        if d == 1:
            return (0.5 * sign) * value
        if d == 2:
            return (0.5 * sign) * y_sign * value
        return sign * yz_sign * edge * value

    def build(rows):
        for part_no in range(2):
            for i in range(3):
                for j in range(3):
                    c = part_no * PAIRS + i * 3 + j
                    flip = part_no * PAIRS + j * 3 + i
                    back = 1.0 if part_no else -1.0
                    for e in rows:
                        wx = wide_link(0, c, e)
                        if e > 0:
                            gauge[0, c, e - 1] = wx
                        if e < 4:
                            gauge[1, flip, e] = back * wx
                        if e == 0:
                            continue
                        wz = wide_link(2, c, e)
                        gauge[3, c, e - 1] = wz
                        gauge[4, flip, e - 1] = back * z_dn(wz)
                        wt = wide_link(3, c, e)
                        gauge[5, c, e - 1] = wt
                        gauge[6, flip, e - 1] = back * roll(wt, 1, 0)
                        wy = wide_link(1, c, e)
                        turned = wide_link(1, flip, e)
                        gauge[2, c, e - 1] = wy + back * roll(turned, NZ, 1)

    build((2, 3))
    for item in near[:2] + far[:2] + far[4:]:
        item.wait()
    build((0, 1, 4))

    def finish_halo(par):
        for item in halo(par):
            item.wait()

    wait_part(0)
    finish_halo(0)
    for c in range(COMPS):
        wide = extend(0, c)
        for e in range(6):
            dirn[c, e] = wide[e]
            resid[c, e] = wide[e]
    norm = fill(summed(0), 0)

    def hop(field, e0):
        total = [None] * COMPS
        terms = (
            (0, lambda c: field[c, e0 + 1:e0 + 3]),
            (1, lambda c: field[c, e0 - 1:e0 + 1]),
            (2, lambda c: roll(field[c, e0:e0 + 2], NZ, 2)),
            (3, lambda c: z_up(field[c, e0:e0 + 2])),
            (4, lambda c: z_dn(field[c, e0:e0 + 2])),
            (5, lambda c: roll(field[c, e0:e0 + 2], -1, 1)),
            (6, lambda c: roll(field[c, e0:e0 + 2], 1, 1)),
        )
        for term, shifted in terms:
            v = [shifted(c) for c in range(COMPS)]
            for i in range(3):
                for j in range(3):
                    wre = gauge[term, i * 3 + j, e0 - 1:e0 + 1]
                    wim = gauge[term, PAIRS + i * 3 + j, e0 - 1:e0 + 1]
                    re = wre * v[j] - wim * v[3 + j]
                    im = wre * v[3 + j] + wim * v[j]
                    total[i] = re if total[i] is None else total[i] + re
                    total[3 + i] = im if total[3 + i] is None else total[3 + i] + im
        return total

    def image_of():
        for e0 in (1, 3):
            for c, value in enumerate(hop(dirn, e0)):
                mid[c, e0:e0 + 2] = value
        image = hop(mid, 2)
        packed = []
        dpack = []
        for c in range(COMPS):
            d2, d3 = dirn[c, 2], dirn[c, 3]
            dp = jnp.where(first, roll(d2, -2, 0), roll(d3, 2, 0))
            wp = jnp.where(first, roll(image[c][0], -2, 0), roll(image[c][1], 2, 0))
            dpack.append(dp)
            packed.append(mass_sq * dp - wp)
        return packed, dpack

    def row(values, k):
        return jnp.broadcast_to(values[k:k + 1], (8, lanes))

    def accumulate(gain):
        for c in range(COMPS):
            total = out_ref[c]
            for k in range(nshift):
                total = total + row(gain, k) * shiftdirs[k, c]
            out_ref[c] = total

    def catch_up(gain, zeta_now, beta_shift):
        accumulate(gain)
        for k in range(nshift):
            zk, bk = row(zeta_now, k), row(beta_shift, k)
            for c in range(COMPS):
                shiftdirs[k, c] = zk * rpack[c] + bk * shiftdirs[k, c]

    def iterate(step, last):
        norm, zeta, zeta_old, alpha_old, beta_old, gain, beta_shift, along, score = [state[k] for k in range(9)]
        par = step % 2 if last else lax.rem(step, 2)
        packed, dpack = image_of()
        res = [rpack[c] for c in range(COMPS)]
        part[par, pl.ds(me, 1)] = dots([inner(dpack, packed), inner(res, packed), inner(packed, packed), inner(spack, res)])[None]
        send_part(par)
        if not last:
            corner_tiles(packed, par)
            for c in range(COMPS):
                ws[par, c] = packed[c]
            for item in halo(par):
                item.start()
        catch_up(gain, zeta, beta_shift)
        wait_part(par)
        sums = summed(par)
        alpha = norm / fill(sums, 0)
        zeta_new = zeta * zeta_old * alpha_old / (
            alpha * beta_old * (zeta_old - zeta) + zeta_old * alpha_old * (1.0 + shift_rows * alpha)
        )
        ratio = zeta_new / zeta
        along = zeta * fill(sums, 3) + beta_shift * along
        gain = residue_rows * alpha * ratio
        score = score + gain * along
        if last:
            return gain, score
        norm_next = norm - 2.0 * alpha * fill(sums, 1) + alpha * alpha * fill(sums, 2)
        beta = norm_next / norm
        beta_shift = beta * ratio * ratio
        finish_halo(par)
        step_a, step_b = row(alpha, 0), row(beta, 0)
        for c in range(COMPS):
            rpack[c] = rpack[c] - step_a * ws[par, c]
            wide = extend(par, c)
            for e in range(6):
                fresh = resid[c, e] - step_a * wide[e]
                resid[c, e] = fresh
                dirn[c, e] = fresh + step_b * dirn[c, e]
        for k, value in enumerate((norm_next, zeta_new, zeta, alpha, beta, gain, beta_shift, along, score)):
            state[k] = value

    one = jnp.ones((16, lanes), jnp.float32)
    none = jnp.zeros((16, lanes), jnp.float32)

    def body(step, carry):
        iterate(step, False)
        return carry

    for k, value in enumerate((norm, one, one, one, none, none, none, none, none)):
        state[k] = value
    lax.fori_loop(1, ITERS, body, 0)
    gain, score = iterate(ITERS, True)
    act[g] = jnp.sum(score, axis=0, keepdims=True)

    def swap(p):
        device = (lax.rem(g + p, n_grp), zt, xy)
        return copy(act.at[g], act.at[g], asend.at[p], arecv.at[g], device)

    def swapped(p):
        there = lax.rem(g + n_grp - p, n_grp)
        return copy(act.at[there], act.at[there], asend.at[p], arecv.at[there], (there, zt, xy))

    for p in range(1, n_grp):
        swap(p).start()
    accumulate(gain)
    for p in range(1, n_grp):
        swapped(p).wait_recv()
        swap(p).wait_send()
    total = act[0]
    for k in range(1, n_grp):
        total = total + act[k]
    sites = n_grp * n_all * cells_x * cells_t * lanes
    action_ref[0] = jnp.max(total) * (1.0 / sites)


def on_device(sizes, source, links, shifts, residues, mass):
    n_grp, n_zt, n_xy = sizes
    cells_x, cells_t, lanes = source.shape[3:]
    n_all = n_zt * n_xy
    f32 = jnp.float32
    tiles = lambda *lead: pltpu.VMEM(lead + (8, lanes), f32)
    rows = lambda count: pltpu.VMEM((count, lanes), f32)
    nshift = shifts.shape[0]
    vmem = pl.BlockSpec(memory_space=pltpu.VMEM)
    smem = pl.BlockSpec(memory_space=pltpu.SMEM)
    dma = pltpu.SemaphoreType.DMA
    rational, action = pl.pallas_call(
        functools.partial(kernel, (n_grp, n_zt, n_xy, cells_x, cells_t)),
        out_shape=(
            jax.ShapeDtypeStruct((COMPS, 8, lanes), f32),
            jax.ShapeDtypeStruct((1,), f32),
        ),
        in_specs=[pl.BlockSpec(memory_space=pl.ANY)] * 2 + [smem] * 3,
        out_specs=(vmem, smem),
        scratch_shapes=[
            tiles(4 * MAT), tiles(2, 4 * MAT), tiles(2, 2 * MAT), tiles(PAIRS), tiles(2, 2 * MAT), tiles(PAIRS),
            rows(40), rows(24), rows(24), rows(40), rows(24), rows(24),
            tiles(7, MAT, 4), tiles(COMPS, 6), tiles(COMPS, 6), tiles(COMPS, 6),
            tiles(nshift, COMPS), tiles(COMPS), tiles(2, COMPS), tiles(2, 4, COMPS),
            tiles(2, 4), tiles(2, 4), pltpu.VMEM((2, n_all, 1, lanes), f32), pltpu.VMEM((n_grp, 1, lanes), f32),
            pltpu.VMEM((9, 16, lanes), f32), tiles(COMPS), tiles(2 * MAT), dma((2,)),
            dma((13,)), dma((13,)), dma((2, 8)), dma((2, 8)),
            dma((2, n_all)), dma((2, n_all)), dma((n_grp,)), dma((n_grp,)),
        ],
        compiler_params=pltpu.CompilerParams(collective_id=0, has_side_effects=True),
    )(
        source.reshape(COMPS, 8, lanes), links.reshape(2 * MAT, 8, lanes), shifts, residues, mass
    )
    return rational.reshape(source.shape), action


def solution(mesh):
    sizes = tuple(mesh.shape[name] for name in ("grp", "zt", "xy"))
    field = P("grp", None, None, "xy", "zt", None)
    return jax.shard_map(
        functools.partial(on_device, sizes),
        mesh=mesh,
        in_specs=(field, P("grp", None, None, None, "xy", "zt", None), P(), P(), P()),
        out_specs=(field, P()),
        check_vma=False,
    )
```
